256 devices in a mesh: mem: 4 (over y), cell: 64 (over x, z, core).
Axes of the slice: x: 4, y: 4, z: 8, core: 2. Of those that a mesh axis runs over, the one named last changes fastest.
Arguments:
- depth: float32 [64, 1048576], P('mem', 'cell'), may hold values from 1 to 3
- discharge: float32 [64, 1048576], P('mem', 'cell'), may hold values from -1.5 to 1.5
- gate: int32 [1048576], P('cell'), may hold values from 0 to 1, as said below
- pump: int32 [2, 1048576], P(None, 'cell'), may hold values 0 or 1
- pump_rate: float32 [1048576], P('cell'), may hold values from 1 to 5
- obs_index: int32 [64, 512], P('cell'), may hold values from 0 to 16383, as said below
- obs_value: float32 [64, 512], P('cell'), may hold values from 1 to 3
- obs_error: float32 [64, 512], P('cell'), may hold values from 0.25 to 1.04
Outputs:
- depth_analysis: float32 [64, 1048576], P('mem', 'cell')
- discharge_analysis: float32 [64, 1048576], P('mem', 'cell')
The draws below stay inside these ranges and needn't reach their ends.
Inputs may be any that keep to these rules, and one draw needn't show every extreme that they name: The gate on the first face of every slab after the first (cells s * 16384 with s >= 1) is open. `obs_index`: the offsets of one slab are distinct.
All inputs are finite; a program needn't handle non-finite values. No bound on the sum of `pump` on one device may be relied on, other than what follows from the above.
Results may differ from the reference program's by a relative error of at most 0.0003.
Values sent between devices are 32-bit elements; how exact they have to be, the bound alone decides.
No kernel may reach another device: no remote copies, remote signals or barrier semaphores. Data moves between devices by JAX's collectives and lax.ppermute only.
A program may use at most 64 MiB of HBM per device.

```python
import math
import jax
import jax.numpy as jnp
from jax import lax

MEMBERS = 64
CELL_DEV = 16384
PER = 512
STEPS = 2
NS_ITERS = 12
SLABS = 64
OBS_SLAB = 512
CELLS = 1048576
UNITS = 2048
NOBS = 32768


def draw_gate(key, part):
    opened = jax.random.randint(jax.random.fold_in(key, 41), (SLABS, CELL_DEV), 0, 4) > 0
    values = opened.astype(jnp.int32)
    values = values.at[:, 0].set(1)
    return values.reshape(-1).astype(jnp.int32)


def draw_obs_index(key, part):
    keys = jax.random.split(jax.random.fold_in(key, 23), SLABS)
    perms = jax.vmap(lambda single: jax.random.permutation(single, CELL_DEV))(keys)
    return perms[:, :OBS_SLAB].astype(jnp.int32)


def draw_obs_error(key, part):
    shape = (SLABS, OBS_SLAB)
    slab_pos = jnp.arange(SLABS, dtype=jnp.float32)[:, None] / max(SLABS - 1, 1)
    growth = jnp.sqrt(1.0 + 2.0 * slab_pos)
    base = jnp.exp(jax.random.uniform(jax.random.fold_in(key, 31), shape, jnp.float32, jnp.log(0.25), jnp.log(0.6)))
    return base * growth


def set_ends(drawn, rng, least, high):
    shape = drawn.shape
    place = [jax.random.randint(jax.random.fold_in(rng, axis), (), 0, shape[axis]) for axis in range(len(shape))]
    drawn = drawn.at[tuple(place)].set(least)
    longest = shape.index(max(shape))
    place[longest] = (place[longest] + 1) % shape[longest]
    return drawn.at[tuple(place)].set(high)


def levels(key, shape, shards, smallest, top_value):
    def one(dim, blocks):
        heights = jax.random.uniform(jax.random.fold_in(jax.random.fold_in(key, 6), dim), (blocks,), jnp.float32, smallest / len(shards), top_value / len(shards))
        return jnp.repeat(jnp.exp(heights), shape[dim] // blocks).reshape((-1,) + (1,) * (len(shape) - dim - 1))

    gain = one(*shards[0])
    for cut in shards[1:]:
        gain = gain * one(*cut)
    return gain


def scatter_about(stream_key, dims, deviation, reach, cuts=(), kind=jnp.bfloat16):
    array = deviation * jax.random.normal(stream_key, dims, jnp.float32)
    if cuts:
        array = array * levels(stream_key, dims, cuts, -0.22, 0.18)
    return jnp.clip(array, -reach, reach).astype(kind)


def setup_inputs(seed: int = 0) -> dict:
    key_list = jax.random.split(jax.random.key(seed), 9)
    return {
        "depth": jnp.clip(1.0 + 2.0 * jax.random.uniform(key_list[0], (MEMBERS, CELLS), jnp.float32) ** levels(key_list[0], (MEMBERS, CELLS), ((0, 4), (1, 64)), -0.2, 0.2), 1.0, 3.0),
        "discharge": scatter_about(key_list[1], (MEMBERS, CELLS), 0.4, 1.5, ((0, 4), (1, 64)), jnp.float32),
        "gate": draw_gate(jax.random.fold_in(key_list[8], 71), 0),
        "pump": set_ends((jax.random.randint(key_list[3], (STEPS, CELLS), 0, 4) < 1).astype(jnp.int32), jax.random.fold_in(key_list[3], 1), 0, 1),
        "pump_rate": jnp.clip(jnp.exp(math.log(5.0) - 1.609438 * jax.random.uniform(key_list[4], (CELLS,), jnp.float32) ** levels(key_list[4], (CELLS,), ((0, 64),), -0.2, 0.2)), 1.0, 5.0),
        "obs_index": draw_obs_index(jax.random.fold_in(key_list[8], 71), 0),
        "obs_value": jnp.clip(1.0 + 2.0 * jax.random.uniform(key_list[6], (SLABS, OBS_SLAB), jnp.float32) ** levels(key_list[6], (SLABS, OBS_SLAB), ((0, 64),), -0.2, 0.2), 1.0, 3.0),
        "obs_error": draw_obs_error(jax.random.fold_in(key_list[8], 71), 0),
    }


gravity = 9.81
step_dt = 0.06

def face_fluxes(depth_left, flow_left, depth_right, flow_right, faces):
    opened = faces > 0.5
    safe_dl = jnp.where(opened, depth_left, 1.0)
    safe_fl = jnp.where(opened, flow_left, 0.0)
    safe_dr = jnp.where(opened, depth_right, 1.0)
    safe_fr = jnp.where(opened, flow_right, 0.0)
    speed_left = safe_fl / safe_dl
    speed_right = safe_fr / safe_dr
    wave_left = jnp.sqrt(gravity * safe_dl)
    wave_right = jnp.sqrt(gravity * safe_dr)
    slowest = jnp.minimum(jnp.minimum(speed_left - wave_left, speed_right - wave_right), 0.0)
    fastest = jnp.maximum(jnp.maximum(speed_left + wave_left, speed_right + wave_right), 0.0)
    moment_left = safe_fl * speed_left + 0.5 * gravity * safe_dl * safe_dl
    moment_right = safe_fr * speed_right + 0.5 * gravity * safe_dr * safe_dr
    spread = fastest - slowest
    mass = (fastest * safe_fl - slowest * safe_fr + slowest * fastest * (safe_dr - safe_dl)) / spread
    moment = (fastest * moment_left - slowest * moment_right + slowest * fastest * (safe_fr - safe_fl)) / spread
    mass = jnp.where(opened, mass, 0.0)
    left_side = jnp.where(opened, moment, 0.5 * gravity * depth_left * depth_left)
    right_side = jnp.where(opened, moment, 0.5 * gravity * depth_right * depth_right)
    return (mass, left_side, right_side)

def advance(depth_pad, flow_pad, faces, inflow):
    mass, left_side, right_side = face_fluxes(depth_pad[..., :-1], flow_pad[..., :-1], depth_pad[..., 1:], flow_pad[..., 1:], faces)
    depth_new = depth_pad[..., 1:-1] - step_dt * (mass[..., 1:] - mass[..., :-1]) + step_dt * inflow
    flow_new = flow_pad[..., 1:-1] - step_dt * (left_side[..., 1:] - right_side[..., :-1])
    return (depth_new, flow_new)

def batch_product(first, second):
    return jnp.einsum('uij,ujk->uik', first, second, precision=lax.Precision.HIGHEST)

def transform_units(grams, cross, factor_rho):
    count = grams.shape[-1]
    identity = jnp.eye(count, dtype=jnp.float32)
    system = identity + factor_rho * factor_rho / (count - 1) * grams
    norm_scale = jnp.sqrt(lax.optimization_barrier(jnp.sum(system * system, axis=(1, 2))))
    iterate = system / norm_scale[:, None, None]
    inverse = jnp.broadcast_to(identity, system.shape)

    def newton_step(turn, carry):
        current, invroot = carry
        factor = 1.5 * identity - 0.5 * batch_product(invroot, current)
        return (batch_product(current, factor), batch_product(factor, invroot))
    iterate, inverse = lax.fori_loop(0, NS_ITERS, newton_step, (iterate, inverse))
    root_weight = inverse / jnp.sqrt(norm_scale)[:, None, None]
    solved = batch_product(inverse, inverse) / norm_scale[:, None, None]
    mean_weight = factor_rho / (count - 1) * jnp.einsum('uij,uj->ui', solved, cross, precision=lax.Precision.HIGHEST)
    return factor_rho * (root_weight + mean_weight[:, :, None])

def reference(depth, discharge, gate, pump, pump_rate, obs_index, obs_value, obs_error):
    inner = gate[1:].astype(jnp.float32)
    faces = jnp.concatenate([jnp.zeros((1,), jnp.float32), inner, jnp.zeros((1,), jnp.float32)])

    def member_run(pair):
        depth_row, flow_row = pair
        for step in range(STEPS):
            inflow = pump_rate * pump[step].astype(jnp.float32)
            depth_row, flow_row = advance(jnp.pad(depth_row, 1), jnp.pad(flow_row, 1), faces, inflow)
        return (depth_row, flow_row)
    depth_fc, flow_fc = lax.map(member_run, (depth, discharge))
    count = depth_fc.shape[0]
    observed = ((jnp.arange(SLABS, dtype=jnp.int32) * CELL_DEV)[:, None] + obs_index).reshape(-1).astype(jnp.int32)
    home = (observed // PER).astype(jnp.int32)
    seen = depth_fc[:, observed]
    seen_mean = lax.optimization_barrier(jnp.mean(seen, axis=0))
    precision_obs = 1.0 / obs_error.reshape(-1)
    scaled = (seen - seen_mean[None, :]) * precision_obs[None, :]
    innov = (obs_value.reshape(-1) - seen_mean) * precision_obs
    total_misfit = jnp.sum(innov * innov)
    total_spread = jnp.sum(scaled * scaled) / (count - 1)
    factor_rho = jnp.sqrt(total_misfit / (total_spread + NOBS))

    def add_slab(carry, slab):
        grams, cross = carry
        block = lax.dynamic_slice_in_dim(scaled, slab * OBS_SLAB, OBS_SLAB, 1)
        innov_block = lax.dynamic_slice_in_dim(innov, slab * OBS_SLAB, OBS_SLAB, 0)
        homes = lax.dynamic_slice_in_dim(home, slab * OBS_SLAB, OBS_SLAB, 0)
        outer = jnp.einsum('ik,jk->kij', block, block, precision=lax.Precision.HIGHEST)
        cross_terms = (block * innov_block[None, :]).T
        for offset in (-1, 0, 1):
            target = homes + offset
            target = jnp.where((target >= 0) & (target < UNITS), target, UNITS).astype(jnp.int32)
            grams = grams + jax.ops.segment_sum(outer, target, num_segments=UNITS + 1)[:UNITS]
            cross = cross + jax.ops.segment_sum(cross_terms, target, num_segments=UNITS + 1)[:UNITS]
        return ((grams, cross), None)
    start = (jnp.zeros((UNITS, count, count), jnp.float32), jnp.zeros((UNITS, count), jnp.float32))
    (grams, cross), _ = lax.scan(add_slab, start, jnp.arange(SLABS, dtype=jnp.int32))
    mixing = transform_units(grams, cross, factor_rho)
    fields = jnp.stack([depth_fc, flow_fc]).reshape(2, count, UNITS, PER)
    field_mean = lax.optimization_barrier(jnp.mean(fields, axis=1, keepdims=True))
    analysed = field_mean + jnp.einsum('fiur,uij->fjur', fields - field_mean, mixing, precision=lax.Precision.HIGHEST)
    restored = analysed.reshape(2, count, CELLS)
    return (restored[0], restored[1])
```

```python
import functools
import jax
import jax.numpy as jnp
from jax import lax
from jax.experimental import pallas as pl
from jax.experimental.pallas import tpu as pltpu
from jax.sharding import PartitionSpec as P

PER = 512
NS_ITERS = 12
gravity = 9.81
step_dt = 0.06
LANE = 128
F32 = jnp.float32
BF16 = jnp.bfloat16


def mm(a, b, dims=((1,), (0,))):
    return lax.dot_general(a, b, (dims, ((), ())), precision=lax.Precision.HIGHEST, preferred_element_type=F32)


def window_step(h, q, gate, inflow):
    back = h.shape[1] - 1
    gh = gravity * h
    u = q * (1.0 / h)
    c = gh * lax.rsqrt(gh)
    slow = u - c
    fast = u + c
    pressure = (0.5 * gh) * h
    moment = q * u + pressure
    hl = pltpu.roll(h, 1, 1)
    ql = pltpu.roll(q, 1, 1)
    a = jnp.minimum(jnp.minimum(pltpu.roll(slow, 1, 1), slow), 0.0)
    b = jnp.maximum(jnp.maximum(pltpu.roll(fast, 1, 1), fast), 0.0)
    ml = pltpu.roll(moment, 1, 1)
    inv = 1.0 / (b - a)
    ab = a * b
    mass = (b * ql - a * q + ab * (h - hl)) * inv
    mom = (b * ml - a * moment + ab * (q - ql)) * inv
    opened = jnp.broadcast_to(gate, h.shape) > 0.5
    opened_next = jnp.broadcast_to(pltpu.roll(gate, back, 1), h.shape) > 0.5
    mass = jnp.where(opened, mass, 0.0)
    right_side = jnp.where(opened, mom, pressure)
    left_side = jnp.where(opened_next, pltpu.roll(mom, back, 1), pressure)
    h_new = h - step_dt * (pltpu.roll(mass, back, 1) - mass) + inflow
    q_new = q - step_dt * (left_side - right_side)
    return h_new, q_new


def forecast_kernel(
    depth, flow, gate, pump, rate, low, high, offsets, *refs
):
    *fields, seen, h0, q0, h1, q1, rows, table = refs
    members, cells = depth.shape
    quarters = len(fields)
    quart = cells // quarters
    pad = 2 * LANE
    total = cells + 2 * pad
    end = pad + cells
    h0[:, pad:end] = depth[...]
    q0[:, pad:end] = flow[...]
    h0[:, pad - LANE : pad] = low[0:members, :]
    q0[:, pad - LANE : pad] = low[members : 2 * members, :]
    h0[:, end : end + LANE] = high[0:members, :]
    q0[:, end : end + LANE] = high[members : 2 * members, :]
    for r in range(2):
        h0[:, r * (total - LANE) : r * (total - LANE) + LANE] = jnp.ones((members, LANE), F32)
        q0[:, r * (total - LANE) : r * (total - LANE) + LANE] = jnp.zeros((members, LANE), F32)
        rows[:, r * (total - LANE) : r * (total - LANE) + LANE] = jnp.zeros((8, LANE), F32)
    rows[0:1, pad:end] = gate[...].astype(F32)
    rows[1:2, pad:end] = step_dt * (rate[...] * pump[0:1, :].astype(F32))
    rows[2:3, pad:end] = step_dt * (rate[...] * pump[1:2, :].astype(F32))
    rows[0:1, pad - LANE : pad] = low[2 * members : 2 * members + 1, :]
    rows[1:2, pad - LANE : pad] = low[2 * members + 1 : 2 * members + 2, :]
    rows[0:1, end : end + LANE] = high[2 * members : 2 * members + 1, :]
    rows[1:2, end : end + LANE] = high[2 * members + 1 : 2 * members + 2, :]
    first = lax.axis_index("cell") == 0
    lane = lax.broadcasted_iota(jnp.int32, (1, LANE), 1)
    shut = jnp.where(first, 1, 0) * jnp.where(lane == 0, 1, 0)
    rows[0:1, pad : pad + LANE] = jnp.where(shut > 0, 0.0, rows[0:1, pad : pad + LANE])

    w1 = 26 * LANE

    def first_step(i, _):
        at = pl.ds(pl.multiple_of(i * w1, LANE), w1 + 2 * LANE)
        h, q = window_step(h0[:, at], q0[:, at], rows[0:1, at], rows[1:2, at])
        put = pl.ds(pl.multiple_of(i * w1 + LANE, LANE), w1)
        h1[:, put] = h[:, LANE : LANE + w1]
        q1[:, put] = q[:, LANE : LANE + w1]
        return 0

    lax.fori_loop(0, (cells + 2 * LANE) // w1, first_step, 0)
    w2 = 16 * LANE
    for k in range(quarters):
        first_tile = lax.rem(lax.axis_index("mem") + k, quarters) * (quart // LANE)

        def second_step(i, _):
            tile = first_tile + i * (w2 // LANE)
            at = pl.ds(pl.multiple_of(pad - LANE + tile * LANE, LANE), w2 + 2 * LANE)
            h, q = window_step(h1[:, at], q1[:, at], rows[0:1, at], rows[2:3, at])
            h = h[:, LANE : LANE + w2]
            put = pl.ds(pl.multiple_of(i * w2, LANE), w2)
            fields[k][0, :, put] = h
            fields[k][1, :, put] = q[:, LANE : LANE + w2]
            for t in range(w2 // LANE):
                table[tile + t] = h[:, t * LANE : (t + 1) * LANE]
            return 0

        lax.fori_loop(0, quart // w2, second_step, 0)
    lanes = lax.broadcasted_iota(jnp.int32, (members, LANE), 1)

    def pick(g, _):
        acc = jnp.zeros((members, LANE), F32)
        for k in range(LANE):
            spot = offsets[g * LANE + k]
            row = table[lax.shift_right_logical(spot, 7)]
            turn = jnp.bitwise_and(k - spot, LANE - 1)
            acc = jnp.where(lanes == k, pltpu.roll(row, turn, 1), acc)
        for m in range(quarters):
            seen[m, :, pl.ds(pl.multiple_of(g * LANE, LANE), LANE)] = acc
        return 0

    lax.fori_loop(0, seen.shape[2] // LANE, pick, 0)


def message_kernel(*refs):
    for end in range(2):
        depth, flow, gate, pump, rate = refs[5 * end : 5 * end + 5]
        out = refs[10 + end]
        n = depth.shape[0]
        out[0:n] = depth[...]
        out[n : 2 * n] = flow[...]
        out[2 * n : 2 * n + 1] = gate[...].astype(F32)
        out[2 * n + 1 : 2 * n + 2] = step_dt * (rate[...] * pump[0:1].astype(F32))
        out[2 * n + 2 :] = jnp.zeros((6, LANE), F32)


def scaled_obs(seen_ref, value, error):
    groups = seen_ref.shape[0]
    mem = lax.axis_index("mem")
    seen = jnp.concatenate([seen_ref[lax.rem(mem + groups - k, groups)] for k in range(groups)], axis=0)
    mean = jnp.mean(seen, axis=0, keepdims=True)
    precision = 1.0 / error
    return (seen - mean) * precision, (value - mean) * precision


def totals_kernel(seen, value, error, offsets, *refs, last):
    totals, edge = refs[3:5]
    scaled, innov = scaled_obs(seen, value[...], error[...])
    members = scaled.shape[0]
    misfit = jnp.sum(innov * innov, axis=(0, 1), keepdims=True)
    spread = jnp.sum(scaled * scaled, axis=(0, 1), keepdims=True) / (members - 1)
    lane = lax.broadcasted_iota(jnp.int32, totals.shape, 1)
    totals[...] = jnp.where(lane == 0, misfit, jnp.where(lane == 1, spread, 0.0))
    upper = lax.axis_index("mem") == lax.axis_size("mem") - 1
    here = jnp.where(upper, 0, last)
    masked = jnp.where(offsets[...] // PER == here, scaled, 0.0)
    extended = jnp.concatenate([scaled, jnp.broadcast_to(innov, (8, innov.shape[1]))], axis=0)
    edge[...] = mm(extended, masked, ((1,), (1,)))


def split(x):
    top = x.astype(BF16)
    rest = x - top.astype(F32)
    middle = rest.astype(BF16)
    return top, middle, (rest - middle.astype(F32)).astype(BF16)


def dot(a, b):
    return lax.dot_general(a, b, (((1,), (0,)), ((), ())), preferred_element_type=F32)


def transform_kernel(seen, value, error, offsets, totals, edge, mixing, weights, *, total_obs):
    scaled, innov = scaled_obs(seen, value[...], error[...])
    members = scaled.shape[0]
    pack = 4
    groups = mixing.shape[0]
    wide = pack * members
    weights[...] = jnp.zeros(weights.shape, BF16)
    extended = jnp.concatenate([scaled, jnp.broadcast_to(innov, (8, innov.shape[1]))], axis=0)
    mem = lax.axis_index("mem")
    polder = offsets[...] // PER - mem * (groups * pack)
    sums = jnp.sum(totals[...], axis=0, keepdims=True)
    lane = lax.broadcasted_iota(jnp.int32, sums.shape, 1)
    misfit = jnp.sum(jnp.where(lane == 0, sums, 0.0), axis=(0, 1), keepdims=True)
    spread = jnp.sum(jnp.where(lane == 1, sums, 0.0), axis=(0, 1), keepdims=True)
    rho2 = misfit / (spread + total_obs)
    rho = jnp.sqrt(rho2)
    r64 = lax.broadcasted_iota(jnp.int32, (members, wide), 0)
    c64 = lax.broadcasted_iota(jnp.int32, (members, wide), 1)
    eye = jnp.where(r64 == c64 % members, 1.0, 0.0)
    half = lax.broadcasted_iota(jnp.int32, (members, LANE), 1) // members
    keep = [jnp.where(half == k, 1.0, 0.0).astype(BF16) for k in range(2)]

    def load_weights(g, parts):
        for p, part in enumerate(parts):
            for k in range(pack):
                cols = slice((k // 2) * LANE, (k // 2 + 1) * LANE)
                weights[g, p, k * members : (k + 1) * members, cols] = part[:, cols] * keep[k % 2]

    def product(g, pieces):
        n = [p[0].shape[0] for p in pieces]
        total = [None] * len(pieces)
        for w, depth in ((2, 1), (1, 2), (0, 3)):
            stack = jnp.concatenate([p[d] for p in pieces for d in range(depth)], axis=0)
            y = dot(stack, weights[g, w])
            at = 0
            for i in range(len(pieces)):
                slabs = [y[at + d * n[i] : at + (d + 1) * n[i]] for d in range(depth)]
                at += depth * n[i]
                piece = slabs[-1]
                for z in reversed(slabs[:-1]):
                    piece = piece + z
                total[i] = piece if total[i] is None else total[i] + piece
        return total

    low_edge = jnp.where(mem == 0, 1.0, 0.0)
    high_edge = jnp.where(mem == lax.axis_size("mem") - 1, 1.0, 0.0)
    wide_edge = jnp.concatenate([edge[...]] * pack, axis=1)
    e_col = lax.broadcasted_iota(jnp.int32, wide_edge.shape, 1) // members
    starts = []
    for g in range(groups):
        picked = jnp.concatenate(
            [jnp.where(jnp.abs(polder - (g * pack + k)) <= 1, scaled, 0.0) for k in range(pack)], axis=0
        )
        gram = mm(extended, picked, ((1,), (1,)))
        if g == 0:
            gram = gram + jnp.where(e_col == 0, wide_edge * low_edge, 0.0)
        if g == groups - 1:
            gram = gram + jnp.where(e_col == pack - 1, wide_edge * high_edge, 0.0)
        system = eye + rho2 / (members - 1) * gram[:members]
        squares = jnp.sum(system * system, axis=0, keepdims=True)
        column = lax.broadcasted_iota(jnp.int32, squares.shape, 1) // members
        norm2 = jnp.zeros_like(squares)
        for k in range(pack):
            here = jnp.where(column == k, squares, 0.0)
            norm2 = jnp.where(column == k, jnp.sum(here, axis=1, keepdims=True), norm2)
        norm = jnp.sqrt(norm2)
        starts.append((system / norm, gram[members : members + 8], norm))

    def iterate(turn, carry):
        out = []
        for g in range(groups):
            energy, inverse = carry[g]
            parts = split(energy)
            load_weights(g, parts)
            square, step = product(g, [parts, split(inverse)])
            factor = 2.25 * eye - 1.5 * energy + 0.25 * square
            out.append((product(g, [split(factor)])[0], 1.5 * inverse - 0.5 * step))
        return tuple(out)

    carry = lax.fori_loop(0, NS_ITERS, iterate, tuple((s[0], eye) for s in starts))
    for g in range(groups):
        _, cross, norm = starts[g]
        inverse = carry[g][1]
        load_weights(g, split(inverse))
        solved = product(g, [split(product(g, [split(cross)])[0])])[0]
        weight = (rho / (members - 1)) * solved[0:1] / norm
        mixing[g] = rho * (inverse / jnp.sqrt(norm) + weight)


def apply_kernel(*refs):
    quarters = len(refs) // 2
    fields, mixing, out = refs[:quarters], refs[quarters], refs[quarters + 1 :]
    _, rows, width = fields[0].shape
    members = quarters * rows
    for u in range(width // PER):
        mix = mixing[u // 4, :, (u % 4) * members : (u % 4 + 1) * members]
        mix_hi = mix.astype(BF16)
        mix_lo = (mix - mix_hi.astype(F32)).astype(BF16)
        left = jnp.concatenate([mix_hi, mix_hi, mix_lo, mix_lo], axis=1)
        cols = slice(u * PER, (u + 1) * PER)
        for f in range(2):
            x = jnp.concatenate([part[f, :, cols] for part in fields], axis=0)
            mean = jnp.mean(x, axis=0, keepdims=True)
            d = x - mean
            d_hi = d.astype(BF16)
            d_lo = (d - d_hi.astype(F32)).astype(BF16)
            y = dot(left, jnp.concatenate([d_hi, d_lo, d_hi, d_lo], axis=0)) + mean
            for k in range(quarters):
                out[k][f, :, cols] = y[k * rows : (k + 1) * rows]


def assemble_kernel(*refs):
    *parts, depth, flow, sems = refs
    quarters = len(parts)
    quart = parts[0].shape[2]
    copies = []
    for k in range(quarters):
        at = lax.rem(lax.axis_index("mem") + k, quarters) * quart
        for f, target in enumerate((depth, flow)):
            to = target.at[:, pl.ds(pl.multiple_of(at, LANE), quart)]
            copies.append(pltpu.make_async_copy(parts[k].at[f], to, sems.at[k, f]))
    for c in copies:
        c.start()
    for c in copies:
        c.wait()


VM = pl.BlockSpec(memory_space=pltpu.VMEM)
SM = pl.BlockSpec(memory_space=pltpu.SMEM)
ANY = pl.BlockSpec(memory_space=pl.ANY)


def vmem(mib):
    return pltpu.CompilerParams(vmem_limit_bytes=mib << 20)


def shards(depth, discharge, gate, pump, pump_rate, obs_index, obs_value, obs_error):
    rows, cells = depth.shape
    quarters = lax.axis_size("mem")
    slabs = lax.axis_size("cell")
    members = rows * quarters
    quart = cells // quarters
    obs = obs_index.shape[1]
    gate_row = gate.reshape(1, cells)
    rate_row = pump_rate.reshape(1, cells)

    tiles = cells // LANE

    def edge_specs(tile):
        return [pl.BlockSpec((n, LANE), lambda i: (0, tile)) for n in (rows, rows, 1, 2, 1)]

    whole = pl.BlockSpec((2 * rows + 8, LANE), lambda i: (0, 0))
    ends = pl.pallas_call(
        message_kernel,
        grid=(1,),
        out_shape=(jax.ShapeDtypeStruct((2 * rows + 8, LANE), F32),) * 2,
        in_specs=edge_specs(tiles - 1) + edge_specs(0),
        out_specs=(whole, whole),
        name="message",
    )(*((depth, discharge, gate_row, pump, rate_row) * 2))
    up = [(i, i + 1) for i in range(slabs - 1)]
    down = [(i + 1, i) for i in range(slabs - 1)]
    low = lax.ppermute(ends[0], "cell", up)
    high = lax.ppermute(ends[1], "cell", down)
    total = cells + 4 * LANE
    block = jax.ShapeDtypeStruct((2, rows, quart), F32)
    own, *sent, seen = pl.pallas_call(
        forecast_kernel,
        out_shape=(block,) * quarters + (jax.ShapeDtypeStruct((quarters, rows, obs), F32),),
        in_specs=[VM] * 7 + [SM],
        out_specs=(VM,) * (quarters + 1),
        scratch_shapes=[pltpu.VMEM((rows, total), F32)] * 4
        + [pltpu.VMEM((8, total), F32), pltpu.VMEM((cells // LANE, rows, LANE), F32)],
        compiler_params=vmem(24),
        name="forecast",
    )(depth, discharge, gate_row, pump, rate_row, low, high, obs_index.reshape(obs))
    seen_all = lax.all_to_all(seen, "mem", split_axis=0, concat_axis=0, tiled=True)
    totals, edge, *sent = pl.pallas_call(
        functools.partial(totals_kernel, last=cells // PER - 1),
        out_shape=(
            jax.ShapeDtypeStruct((slabs, LANE), F32),
            jax.ShapeDtypeStruct((members + 8, members), F32),
        )
        + (block,) * 3,
        in_specs=[VM, VM, VM, VM, ANY, ANY, ANY],
        out_specs=(VM, VM, ANY, ANY, ANY),
        input_output_aliases={4: 2, 5: 3, 6: 4},
        compiler_params=vmem(8),
        name="totals",
    )(seen_all, obs_value, obs_error, obs_index, *sent)

    def turned(x, by):
        return lax.ppermute(x, "mem", [(i, (i + by) % quarters) for i in range(quarters)])

    moved = [own] + [turned(x, k) for k, x in enumerate(sent, 1)]
    top = quarters - 1
    pairs = [(i, i + 1) for i in range(slabs - 1)]
    pairs += [(top * slabs + i + 1, top * slabs + i) for i in range(slabs - 1)]
    edge = lax.ppermute(edge, ("mem", "cell"), pairs)
    everyone = lax.all_to_all(totals, "cell", split_axis=0, concat_axis=0, tiled=True)
    groups = quart // PER // 4
    mixing = pl.pallas_call(
        functools.partial(transform_kernel, total_obs=float(obs * slabs)),
        out_shape=jax.ShapeDtypeStruct((groups, members, 4 * members), F32),
        in_specs=[VM] * 6,
        out_specs=VM,
        scratch_shapes=[pltpu.VMEM((groups, 3, 4 * members, 4 * members), BF16)],
        compiler_params=vmem(12),
        name="transform",
    )(seen_all, obs_value, obs_error, obs_index, everyone, edge)
    kept, *given = pl.pallas_call(
        apply_kernel,
        out_shape=(block,) * quarters,
        in_specs=[VM] * (quarters + 1),
        out_specs=(VM,) * quarters,
        compiler_params=vmem(14),
        name="apply",
    )(*moved, mixing)
    parts = [kept] + [turned(x, -k) for k, x in enumerate(given, 1)]
    out = jax.ShapeDtypeStruct((rows, cells), F32)
    return pl.pallas_call(
        assemble_kernel,
        out_shape=(out, out),
        in_specs=[VM] * quarters,
        out_specs=(pl.BlockSpec(memory_space=pltpu.HBM),) * 2,
        scratch_shapes=[pltpu.SemaphoreType.DMA((quarters, 2))],
        compiler_params=vmem(10),
        name="assemble",
    )(*parts)


def solution(mesh):
    return jax.shard_map(
        shards,
        mesh=mesh,
        in_specs=(
            P("mem", "cell"),
            P("mem", "cell"),
            P("cell"),
            P(None, "cell"),
            P("cell"),
            P("cell", None),
            P("cell", None),
            P("cell", None),
        ),
        out_specs=(P("mem", "cell"), P("mem", "cell")),
        check_vma=False,
    )
```

```python
import functools
import jax
import jax.numpy as jnp
from jax import lax
from jax.experimental import pallas as pl
from jax.experimental.pallas import tpu as pltpu
from jax.sharding import PartitionSpec as P

PER = 512
NS_ITERS = 12
FULL_ITERS = 6
PACK = 4
gravity = 9.81
step_dt = 0.06
LANE = 128
F32 = jnp.float32
BF16 = jnp.bfloat16


def mm(a, b, dims=((1,), (0,))):
    return lax.dot_general(a, b, (dims, ((), ())), precision=lax.Precision.HIGHEST, preferred_element_type=F32)


def window_step(h, q, gate, inflow):
    back = h.shape[1] - 1
    gh = gravity * h
    u = q * (1.0 / h)
    c = gh * lax.rsqrt(gh)
    slow = u - c
    fast = u + c
    pressure = (0.5 * gh) * h
    moment = q * u + pressure
    hl = pltpu.roll(h, 1, 1)
    ql = pltpu.roll(q, 1, 1)
    a = jnp.minimum(jnp.minimum(pltpu.roll(slow, 1, 1), slow), 0.0)
    b = jnp.maximum(jnp.maximum(pltpu.roll(fast, 1, 1), fast), 0.0)
    ml = pltpu.roll(moment, 1, 1)
    inv = 1.0 / (b - a)
    share = a * inv
    mass = ql - share * ((q - ql) - b * (h - hl))
    mom = ml - share * ((moment - ml) - b * (q - ql))
    opened = jnp.broadcast_to(gate, h.shape) > 0.5
    opened_next = jnp.broadcast_to(pltpu.roll(gate, back, 1), h.shape) > 0.5
    mass = jnp.where(opened, mass, 0.0)
    right_side = jnp.where(opened, mom, pressure)
    left_side = jnp.where(opened_next, pltpu.roll(mom, back, 1), pressure)
    h_new = h - step_dt * (pltpu.roll(mass, back, 1) - mass) + inflow
    q_new = q - step_dt * (left_side - right_side)
    return h_new, q_new


def forecast_kernel(
    depth, flow, gate, pump, rate, low, high, value, error, offsets, *refs
):
    *fields, seen, obs_rows, h0, q0, h1, q1, rows, table = refs
    obs_rows[0:1] = value[...]
    obs_rows[1:2] = 1.0 / error[...]
    obs_rows[2:] = jnp.zeros((6, value.shape[1]), F32)
    members, cells = depth.shape
    quarters = len(fields)
    quart = cells // quarters
    pad = 2 * LANE
    total = cells + 2 * pad
    end = pad + cells
    h0[:, pad:end] = depth[...]
    q0[:, pad:end] = flow[...]
    h0[:, pad - LANE : pad] = low[0:members, :]
    q0[:, pad - LANE : pad] = low[members : 2 * members, :]
    h0[:, end : end + LANE] = high[0:members, :]
    q0[:, end : end + LANE] = high[members : 2 * members, :]
    for r in range(2):
        h0[:, r * (total - LANE) : r * (total - LANE) + LANE] = jnp.ones((members, LANE), F32)
        q0[:, r * (total - LANE) : r * (total - LANE) + LANE] = jnp.zeros((members, LANE), F32)
        rows[:, r * (total - LANE) : r * (total - LANE) + LANE] = jnp.zeros((8, LANE), F32)
    rows[0:1, pad:end] = gate[...].astype(F32)
    rows[1:2, pad:end] = step_dt * (rate[...] * pump[0:1, :].astype(F32))
    rows[2:3, pad:end] = step_dt * (rate[...] * pump[1:2, :].astype(F32))
    rows[0:1, pad - LANE : pad] = low[2 * members : 2 * members + 1, :]
    rows[1:2, pad - LANE : pad] = low[2 * members + 1 : 2 * members + 2, :]
    rows[0:1, end : end + LANE] = high[2 * members : 2 * members + 1, :]
    rows[1:2, end : end + LANE] = high[2 * members + 1 : 2 * members + 2, :]
    first = lax.axis_index("cell") == 0
    lane = lax.broadcasted_iota(jnp.int32, (1, LANE), 1)
    shut = jnp.where(first, 1, 0) * jnp.where(lane == 0, 1, 0)
    rows[0:1, pad : pad + LANE] = jnp.where(shut > 0, 0.0, rows[0:1, pad : pad + LANE])

    w1 = 65 * LANE

    def first_step(i, _):
        at = pl.ds(pl.multiple_of(i * w1, LANE), w1 + 2 * LANE)
        h, q = window_step(h0[:, at], q0[:, at], rows[0:1, at], rows[1:2, at])
        put = pl.ds(pl.multiple_of(i * w1 + LANE, LANE), w1)
        h1[:, put] = h[:, LANE : LANE + w1]
        q1[:, put] = q[:, LANE : LANE + w1]
        return 0

    lax.fori_loop(0, (cells + 2 * LANE) // w1, first_step, 0)
    w2 = 32 * LANE
    for k in range(quarters):
        first_tile = lax.rem(lax.axis_index("mem") + k, quarters) * (quart // LANE)

        def second_step(i, _):
            tile = first_tile + i * (w2 // LANE)
            at = pl.ds(pl.multiple_of(pad - LANE + tile * LANE, LANE), w2 + 2 * LANE)
            h, q = window_step(h1[:, at], q1[:, at], rows[0:1, at], rows[2:3, at])
            h = h[:, LANE : LANE + w2]
            put = pl.ds(pl.multiple_of(i * w2, LANE), w2)
            fields[k][0, :, put] = h
            fields[k][1, :, put] = q[:, LANE : LANE + w2]
            for t in range(w2 // LANE):
                table[tile + t] = h[:, t * LANE : (t + 1) * LANE]
            return 0

        lax.fori_loop(0, quart // w2, second_step, 0)
    lanes = lax.broadcasted_iota(jnp.int32, (members, LANE), 1)

    def pick(g, _):
        acc = jnp.zeros((members, LANE), F32)
        for k in range(LANE):
            spot = offsets[g * LANE + k]
            row = table[lax.shift_right_logical(spot, 7)]
            turn = jnp.bitwise_and(k - spot, LANE - 1)
            acc = jnp.where(lanes == k, pltpu.roll(row, turn, 1), acc)
        for m in range(quarters):
            seen[m, :, pl.ds(pl.multiple_of(g * LANE, LANE), LANE)] = acc
        return 0

    lax.fori_loop(0, seen.shape[2] // LANE, pick, 0)


def message_kernel(*refs):
    for end in range(2):
        depth, flow, gate, pump, rate = refs[5 * end : 5 * end + 5]
        out = refs[10 + end]
        n = depth.shape[0]
        out[0:n] = depth[...]
        out[n : 2 * n] = flow[...]
        out[2 * n : 2 * n + 1] = gate[...].astype(F32)
        out[2 * n + 1 : 2 * n + 2] = step_dt * (rate[...] * pump[0:1].astype(F32))
        out[2 * n + 2 :] = jnp.zeros((6, LANE), F32)


def scaled_obs(seen_ref, obs_rows):
    groups = seen_ref.shape[0]
    mem = lax.axis_index("mem")
    seen = jnp.concatenate([seen_ref[lax.rem(mem + groups - k, groups)] for k in range(groups)], axis=0)
    mean = jnp.mean(seen, axis=0, keepdims=True)
    value = obs_rows[0:1]
    precision = obs_rows[1:2]
    return (seen - mean) * precision, (value - mean) * precision


def totals_kernel(seen, obs_rows, offsets, *refs, last):
    totals, edge = refs[3:5]
    scaled, innov = scaled_obs(seen, obs_rows)
    members = scaled.shape[0]
    misfit = jnp.sum(innov * innov, axis=(0, 1), keepdims=True)
    spread = jnp.sum(scaled * scaled, axis=(0, 1), keepdims=True) / (members - 1)
    lane = lax.broadcasted_iota(jnp.int32, totals.shape, 1)
    totals[...] = jnp.where(lane == 0, misfit, jnp.where(lane == 1, spread, 0.0))
    upper = lax.axis_index("mem") == lax.axis_size("mem") - 1
    here = jnp.where(upper, 0, last)
    masked = jnp.where(offsets[...] // PER == here, scaled, 0.0)
    extended = jnp.concatenate([scaled, jnp.broadcast_to(innov, (8, innov.shape[1]))], axis=0)
    edge[...] = mm(extended, masked, ((1,), (1,)))


def split(x):
    top = x.astype(BF16)
    rest = x - top.astype(F32)
    middle = rest.astype(BF16)
    return top, middle, (rest - middle.astype(F32)).astype(BF16)


def dot(a, b):
    return lax.dot_general(a, b, (((1,), (0,)), ((), ())), preferred_element_type=F32)


def gram_kernel(seen, obs_rows, offsets, grams):
    groups = grams.shape[0]
    scaled, innov = scaled_obs(seen, obs_rows)
    extended = jnp.concatenate([scaled, jnp.broadcast_to(innov, (8, innov.shape[1]))], axis=0)
    polder = offsets[...] // PER - lax.axis_index("mem") * (groups * PACK)
    for g in range(groups):
        picked = [jnp.where(jnp.abs(polder - (g * PACK + k)) <= 1, scaled, 0.0) for k in range(PACK)]
        grams[g] = mm(extended, jnp.concatenate(picked, axis=0), ((1,), (1,)))


def transform_kernel(grams, totals, edge, mixing, weights, *, total_obs):
    groups = mixing.shape[0]
    members, wide = mixing.shape[1:]
    weights[...] = jnp.zeros(weights.shape, BF16)
    sums = jnp.sum(totals[...], axis=0, keepdims=True)
    lane = lax.broadcasted_iota(jnp.int32, sums.shape, 1)
    misfit = jnp.sum(jnp.where(lane == 0, sums, 0.0), axis=(0, 1), keepdims=True)
    spread = jnp.sum(jnp.where(lane == 1, sums, 0.0), axis=(0, 1), keepdims=True)
    rho2 = misfit / (spread + total_obs)
    rho = jnp.sqrt(rho2)
    r64 = lax.broadcasted_iota(jnp.int32, (members, wide), 0)
    c64 = lax.broadcasted_iota(jnp.int32, (members, wide), 1)
    eye = jnp.where(r64 == c64 % members, 1.0, 0.0)
    keep = [jnp.where(c64 // members == k, 1.0, 0.0).astype(BF16) for k in range(PACK)]

    def load_weights(g, parts):
        for p, part in enumerate(parts):
            for k in range(PACK):
                cols = slice((k // 2) * LANE, (k // 2 + 1) * LANE)
                row = p * wide + k * members
                weights[g, row : row + members, cols] = part[:, cols] * keep[k][:, cols]

    def product(g, pieces, full=True):
        n = [p[0].shape[0] for p in pieces]
        total = [None] * len(pieces)
        for w, depth in ((2, 1), (1, 2), (0, 3)) if full else ((1, 1), (0, 2)):
            stack = jnp.concatenate([p[d] for p in pieces for d in range(depth)], axis=0)
            y = dot(stack, weights[g, w * wide : (w + 1) * wide])
            at = 0
            for i in range(len(pieces)):
                piece = y[at + (depth - 1) * n[i] : at + depth * n[i]]
                for d in reversed(range(depth - 1)):
                    piece = piece + y[at + d * n[i] : at + (d + 1) * n[i]]
                at += depth * n[i]
                total[i] = piece if total[i] is None else total[i] + piece
        return total

    mem = lax.axis_index("mem")
    low_edge = jnp.where(mem == 0, 1.0, 0.0)
    high_edge = jnp.where(mem == lax.axis_size("mem") - 1, 1.0, 0.0)
    wide_edge = jnp.concatenate([edge[...]] * PACK, axis=1)
    e_col = lax.broadcasted_iota(jnp.int32, wide_edge.shape, 1) // members
    starts = []
    for g in range(groups):
        gram = grams[g]
        if g == 0:
            gram = gram + jnp.where(e_col == 0, wide_edge * low_edge, 0.0)
        if g == groups - 1:
            gram = gram + jnp.where(e_col == PACK - 1, wide_edge * high_edge, 0.0)
        system = eye + rho2 / (members - 1) * gram[:members]
        squares = jnp.sum(system * system, axis=0, keepdims=True)
        column = lax.broadcasted_iota(jnp.int32, squares.shape, 1) // members
        norm2 = jnp.zeros_like(squares)
        for k in range(PACK):
            here = jnp.where(column == k, squares, 0.0)
            norm2 = jnp.where(column == k, jnp.sum(here, axis=1, keepdims=True), norm2)
        norm = jnp.sqrt(norm2)
        starts.append((system / norm, gram[members : members + 8], norm))

    def iterate(full, turn, carry):
        out = []
        for g in range(groups):
            energy, inverse = carry[g]
            parts = split(energy)
            load_weights(g, parts)
            square, step = product(g, [parts, split(inverse)], full)
            factor = 2.25 * eye - 1.5 * energy + 0.25 * square
            out.append((product(g, [split(factor)], full)[0], 1.5 * inverse - 0.5 * step))
        return tuple(out)

    carry = tuple((s[0], eye) for s in starts)
    carry = lax.fori_loop(0, FULL_ITERS, functools.partial(iterate, True), carry)
    carry = lax.fori_loop(FULL_ITERS, NS_ITERS, functools.partial(iterate, False), carry)
    for g in range(groups):
        _, cross, norm = starts[g]
        inverse = carry[g][1]
        load_weights(g, split(inverse))
        solved = product(g, [split(product(g, [split(cross)])[0])])[0]
        weight = (rho / (members - 1)) * solved[0:1] / norm
        mixing[g] = rho * (inverse / jnp.sqrt(norm) + weight)


def apply_kernel(*refs):
    quarters = len(refs) // 2
    fields, mixing, out = refs[:quarters], refs[quarters], refs[quarters + 1 :]
    _, rows, width = fields[0].shape
    members = quarters * rows
    for u in range(width // PER):
        mix = mixing[u // PACK, :, (u % PACK) * members : (u % PACK + 1) * members]
        mix_hi = mix.astype(BF16)
        mix_lo = (mix - mix_hi.astype(F32)).astype(BF16)
        left = jnp.concatenate([mix_hi, mix_hi, mix_lo, mix_lo], axis=1)
        cols = slice(u * PER, (u + 1) * PER)
        for f in range(2):
            x = jnp.concatenate([part[f, :, cols] for part in fields], axis=0)
            mean = jnp.mean(x, axis=0, keepdims=True)
            d = x - mean
            d_hi = d.astype(BF16)
            d_lo = (d - d_hi.astype(F32)).astype(BF16)
            y = dot(left, jnp.concatenate([d_hi, d_lo, d_hi, d_lo], axis=0)) + mean
            for k in range(quarters):
                out[k][f, :, cols] = y[k * rows : (k + 1) * rows]


def assemble_kernel(*refs):
    *parts, depth, flow, sems = refs
    quarters = len(parts)
    quart = parts[0].shape[2]
    copies = []
    for k in range(quarters):
        at = lax.rem(lax.axis_index("mem") + k, quarters) * quart
        for f, target in enumerate((depth, flow)):
            to = target.at[:, pl.ds(pl.multiple_of(at, LANE), quart)]
            copies.append(pltpu.make_async_copy(parts[k].at[f], to, sems.at[k, f]))
    for c in copies:
        c.start()
    for c in copies:
        c.wait()


VM = pl.BlockSpec(memory_space=pltpu.VMEM)
SM = pl.BlockSpec(memory_space=pltpu.SMEM)
ANY = pl.BlockSpec(memory_space=pl.ANY)


def vmem(mib):
    return pltpu.CompilerParams(vmem_limit_bytes=mib << 20)


def shards(depth, discharge, gate, pump, pump_rate, obs_index, obs_value, obs_error):
    rows, cells = depth.shape
    quarters = lax.axis_size("mem")
    slabs = lax.axis_size("cell")
    members = rows * quarters
    quart = cells // quarters
    obs = obs_index.shape[1]
    gate_row = gate.reshape(1, cells)
    rate_row = pump_rate.reshape(1, cells)

    tiles = cells // LANE

    def edge_specs(tile):
        return [pl.BlockSpec((n, LANE), lambda i: (0, tile)) for n in (rows, rows, 1, 2, 1)]

    whole = pl.BlockSpec((2 * rows + 8, LANE), lambda i: (0, 0))
    ends = pl.pallas_call(
        message_kernel,
        grid=(1,),
        out_shape=(jax.ShapeDtypeStruct((2 * rows + 8, LANE), F32),) * 2,
        in_specs=edge_specs(tiles - 1) + edge_specs(0),
        out_specs=(whole, whole),
        name="message",
    )(*((depth, discharge, gate_row, pump, rate_row) * 2))
    up = [(i, i + 1) for i in range(slabs - 1)]
    down = [(i + 1, i) for i in range(slabs - 1)]
    low = lax.ppermute(ends[0], "cell", up)
    high = lax.ppermute(ends[1], "cell", down)
    total = cells + 4 * LANE
    block = jax.ShapeDtypeStruct((2, rows, quart), F32)
    own, *sent, seen, obs_rows = pl.pallas_call(
        forecast_kernel,
        out_shape=(block,) * quarters + (jax.ShapeDtypeStruct((quarters, rows, obs), F32), jax.ShapeDtypeStruct((8, obs), F32)),
        in_specs=[VM] * 9 + [SM],
        out_specs=(VM,) * (quarters + 2),
        scratch_shapes=[pltpu.VMEM((rows, total), F32)] * 4
        + [pltpu.VMEM((8, total), F32), pltpu.VMEM((cells // LANE, rows, LANE), F32)],
        compiler_params=vmem(24),
        name="forecast",
    )(depth, discharge, gate_row, pump, rate_row, low, high, obs_value, obs_error, obs_index.reshape(obs))
    seen_all = lax.all_to_all(seen, "mem", split_axis=0, concat_axis=0, tiled=True)
    totals, edge, *sent = pl.pallas_call(
        functools.partial(totals_kernel, last=cells // PER - 1),
        out_shape=(
            jax.ShapeDtypeStruct((slabs, LANE), F32),
            jax.ShapeDtypeStruct((members + 8, members), F32),
        )
        + (block,) * 3,
        in_specs=[VM, VM, VM, ANY, ANY, ANY],
        out_specs=(VM, VM, ANY, ANY, ANY),
        input_output_aliases={3: 2, 4: 3, 5: 4},
        compiler_params=vmem(8),
        name="totals",
    )(seen_all, obs_rows, obs_index, *sent)

    def turned(x, by):
        return lax.ppermute(x, "mem", [(i, (i + by) % quarters) for i in range(quarters)])

    moved = [own] + [turned(x, k) for k, x in enumerate(sent, 1)]
    top = quarters - 1
    pairs = [(i, i + 1) for i in range(slabs - 1)]
    pairs += [(top * slabs + i + 1, top * slabs + i) for i in range(slabs - 1)]
    edge = lax.ppermute(edge, ("mem", "cell"), pairs)
    everyone = lax.all_to_all(totals, "cell", split_axis=0, concat_axis=0, tiled=True)
    groups = quart // PER // PACK
    wide = PACK * members
    grams = pl.pallas_call(
        gram_kernel,
        out_shape=jax.ShapeDtypeStruct((groups, members + 8, wide), F32),
        in_specs=[VM] * 3,
        out_specs=VM,
        compiler_params=vmem(10),
        name="gram",
    )(seen_all, obs_rows, obs_index)
    mixing = pl.pallas_call(
        functools.partial(transform_kernel, total_obs=float(obs * slabs)),
        out_shape=jax.ShapeDtypeStruct((groups, members, wide), F32),
        in_specs=[VM] * 3,
        out_specs=VM,
        scratch_shapes=[pltpu.VMEM((groups, 3 * wide, wide), BF16)],
        compiler_params=vmem(12),
        name="transform",
    )(grams, everyone, edge)
    kept, *given = pl.pallas_call(
        apply_kernel,
        out_shape=(block,) * quarters,
        in_specs=[VM] * (quarters + 1),
        out_specs=(VM,) * quarters,
        compiler_params=vmem(14),
        name="apply",
    )(*moved, mixing)
    parts = [kept] + [turned(x, -k) for k, x in enumerate(given, 1)]
    out = jax.ShapeDtypeStruct((rows, cells), F32)
    return pl.pallas_call(
        assemble_kernel,
        out_shape=(out, out),
        in_specs=[VM] * quarters,
        out_specs=(pl.BlockSpec(memory_space=pltpu.HBM),) * 2,
        scratch_shapes=[pltpu.SemaphoreType.DMA((quarters, 2))],
        compiler_params=vmem(10),
        name="assemble",
    )(*parts)


def solution(mesh):
    return jax.shard_map(
        shards,
        mesh=mesh,
        in_specs=(
            P("mem", "cell"),
            P("mem", "cell"),
            P("cell"),
            P(None, "cell"),
            P("cell"),
            P("cell", None),
            P("cell", None),
            P("cell", None),
        ),
        out_specs=(P("mem", "cell"), P("mem", "cell")),
        check_vma=False,
    )
```
